32 devices in a mesh: rows: 8 (over z, y), grp: 4 (over x, core).
Axes of the slice: x: 2, y: 2, z: 4, core: 2. Of those that a mesh axis runs over, the one named last changes fastest.
Arguments:
- rhs: float32 [3, 8, 4, 2, 512], P(None, 'rows', 'grp'), may hold values from -6 to 6
- diag_inverse: bfloat16 [3, 8, 4, 512, 512], P(None, 'rows', 'grp'), as said below
- coupling: bfloat16 [3, 8, 4, 512, 512], P(None, 'rows', 'grp'), may hold values from -0.125 to 0.125
- off_block: bfloat16 [2, 8, 4, 512, 512], P(None, 'rows', 'grp'), may hold values from -0.1875 to 0.1875
- off_route: int32 [2, 8, 4], P(None, 'rows', 'grp'), may hold values from 0 to 15, as said below
Outputs:
- solution: float32 [3, 8, 4, 2, 512], P(None, 'rows', 'grp')
The draws below stay inside these ranges and needn't reach their ends.
Inputs may be any that keep to these rules, and one draw needn't show every extreme that they name: `off_route`: for a block of super-level l the value is s * 8 + t with 0 <= s <= 1 - l: the block belongs to block row t of the same group in super-level l + 1 + s. `diag_inverse`: each matrix is a dominant diagonal plus independent off-diagonal entries.
All inputs are finite; a program needn't handle non-finite values.
Results may differ from the reference program's by a relative error of at most 0.0045.
Values may be sent and summed in bfloat16 or wider, within the bound.
No kernel may reach another device: no remote copies, remote signals or barrier semaphores. Data moves between devices by JAX's collectives and lax.ppermute only.
A program may use at most 64 MiB of HBM per device.

```python
import math
import jax
import jax.numpy as jnp
from jax import lax

B = 512
NRHS = 2
LEVELS = 3
ROWBLOCKS = 8
GROUPS = 4


def draw_diag_inverse(key, part):
    dims_shape = (LEVELS, ROWBLOCKS, GROUPS, B, B)
    first_key, second_key = jax.random.split(jax.random.fold_in(key, 11))
    diagonal = jax.random.uniform(first_key, dims_shape[:4], jnp.float32, 0.5, 1.5)
    random_part = 0.6 / math.sqrt(B) * jax.random.normal(second_key, dims_shape, jnp.float32)
    identity_matrix = jnp.eye(B, dtype=jnp.float32)
    return (random_part + diagonal[..., None] * identity_matrix).astype(jnp.bfloat16)


def draw_off_route(key, part):
    dims_shape = (LEVELS - 1, ROWBLOCKS, GROUPS)
    first_key, second_key = jax.random.split(jax.random.fold_in(key, 23))
    ahead_limit = LEVELS - 1 - jnp.arange(LEVELS - 1, dtype=jnp.int32)
    level_skip = jax.random.randint(first_key, dims_shape, 0, 1 << 20, dtype=jnp.int32) % ahead_limit[:, None, None]
    target_row = jax.random.randint(second_key, dims_shape, 0, ROWBLOCKS, dtype=jnp.int32)
    return (level_skip * ROWBLOCKS + target_row).astype(jnp.int32)


def steps_of(own_key, extent, cuts, smallest, largest):
    def one(dim, blocks):
        heights = jax.random.uniform(jax.random.fold_in(jax.random.fold_in(own_key, 6), dim), (blocks,), jnp.float32, smallest / len(cuts), largest / len(cuts))
        return jnp.repeat(jnp.exp(heights), extent[dim] // blocks).reshape((-1,) + (1,) * (len(extent) - dim - 1))

    level = one(*cuts[0])
    for cut in cuts[1:]:
        level = level * one(*cut)
    return level


def bell_draw(stream_key, dims, deviation, most, cuts=(), held_as=jnp.bfloat16):
    factor_of = steps_of(stream_key, dims, cuts, -0.22, 0.18) if cuts else 1.0
    array = jax.random.normal(stream_key, dims, jnp.float32) * deviation * factor_of
    return jnp.minimum(jnp.maximum(array, -most), most).astype(held_as)


def setup_inputs(seed: int = 0) -> dict:
    key_of = jax.random.split(jax.random.key(seed), 6)
    rhs = bell_draw(key_of[0], (LEVELS, ROWBLOCKS, GROUPS, NRHS, B), 1.0, 6.0, ((1, 8), (2, 4)), jnp.float32)
    diag_inverse = draw_diag_inverse(jax.random.fold_in(key_of[5], 71), 0)
    coupling = bell_draw(key_of[2], (LEVELS, ROWBLOCKS, GROUPS, B, B), (4 * B) ** -0.5, 0.125, ((1, 8), (2, 4)))
    off_block = bell_draw(key_of[3], (LEVELS - 1, ROWBLOCKS, GROUPS, B, B), (2 * B) ** -0.5, 0.1875, ((1, 8), (2, 4)))
    off_route = draw_off_route(jax.random.fold_in(key_of[5], 71), 0)
    return dict(rhs=rhs, diag_inverse=diag_inverse, coupling=coupling, off_block=off_block, off_route=off_route)


def reference(rhs, diag_inverse, coupling, off_block, off_route):
    highest = lax.Precision.HIGHEST
    incoming = jnp.zeros(rhs.shape, jnp.float32)
    group_index = jnp.arange(GROUPS, dtype=jnp.int32)[None, :]
    results = []
    for super_level in range(LEVELS):
        source = rhs[super_level] - incoming[super_level]
        inverse = diag_inverse[super_level]
        coupler = coupling[super_level]
        columns = []
        previous = None
        for group_number in range(GROUPS):
            partial_rhs = source[:, group_number]
            if previous is not None:
                partial_rhs = partial_rhs - jnp.einsum("rkb,rbc->rkc", previous, coupler[:, group_number].astype(jnp.float32), precision=highest)
            previous = jnp.einsum("rkb,rbc->rkc", partial_rhs, inverse[:, group_number].astype(jnp.float32), precision=highest)
            columns.append(previous)
        solved = jnp.stack(columns, axis=1)
        results.append(solved)
        if super_level < LEVELS - 1:
            rounded = lax.optimization_barrier(solved.astype(jnp.bfloat16)).astype(jnp.float32)
            contribution = jnp.einsum("rgkb,rgbc->rgkc", rounded, off_block[super_level].astype(jnp.float32), precision=highest)
            contribution = lax.optimization_barrier(contribution.astype(jnp.bfloat16)).astype(jnp.float32)
            routing = off_route[super_level]
            level_skip = routing // ROWBLOCKS
            target_row = routing % ROWBLOCKS
            incoming = incoming.at[super_level + 1 + level_skip, target_row, group_index].add(contribution)
    return jnp.stack(results, axis=0)
```

```python
import jax
import jax.numpy as jnp
from jax import lax
from jax.sharding import PartitionSpec as P

INNER = 2


def product(x, w):
    high = x.astype(jnp.bfloat16)
    low = (x - high.astype(jnp.float32)).astype(jnp.bfloat16)
    both = jnp.dot(jnp.concatenate([high, low], axis=0), w, preferred_element_type=jnp.float32)
    return both[: x.shape[0]] + both[x.shape[0] :]


def shards(rhs, diag_inverse, coupling, off_block, off_route):
    axes = ("rows", "grp")
    levels, nrhs, width = rhs.shape[0], rhs.shape[3], rhs.shape[4]
    groups, rowblocks = lax.axis_size("grp"), lax.axis_size("rows")
    outer = groups // INNER
    group = lax.axis_index("grp")
    chip, core = group // INNER, group % INNER
    first = core == 0
    source_all = rhs[:, 0, 0]
    inverse, coupler, blocks = diag_inverse[:, 0, 0], coupling[:, 0, 0], off_block[:, 0, 0]
    routes = off_route[:, 0, 0]

    flip = [(g, g ^ 1) for g in range(groups)]
    straight = [(g, (g + INNER) % groups) for g in range(groups)]
    cross = [(g, (g ^ 1) + INNER if (g ^ 1) + INNER < groups else (g ^ 1) + INNER - groups) for g in range(groups)]

    u = product(source_all[0], inverse[0])
    swapped = lax.ppermute(jnp.concatenate([u[None], source_all[1:]], axis=0), "grp", flip)
    inverse_p = lax.ppermute(inverse, "grp", flip)
    coupler_p = lax.ppermute(coupler, "grp", flip)

    device = jnp.arange(rowblocks * groups, dtype=jnp.int32)
    to_row, to_chip = device // groups, (device % groups) // INNER
    results, held = [], None
    incoming = [None] * levels
    for level in range(levels):
        if level == 0:
            u_own, u_other = u, swapped[0]
        else:
            own = jnp.where(first, incoming[level][0], incoming[level][1])
            other = jnp.where(first, incoming[level][1], incoming[level][0])
            u_own = product(source_all[level] - own, inverse[level])
            u_other = product(swapped[level] - other, inverse_p[level])
        z = jnp.where(first, 0.0, u_other)
        solved = u_own - product(product(z, coupler[level]), inverse[level])
        for repeat in range(outer - 1):
            a = lax.ppermute(solved, "grp", cross)
            b = lax.ppermute(solved, "grp", straight)
            before = jnp.where(chip == 0, 0.0, jnp.where(first, a, b))
            z = jnp.where(first, before, u_other - product(product(before, coupler_p[level]), inverse_p[level]))
            solved = u_own - product(product(z, coupler[level]), inverse[level])
        results.append(solved)
        if level < levels - 1:
            contribution = jnp.dot(
                solved.astype(jnp.bfloat16), blocks[level], preferred_element_type=jnp.float32
            ).astype(jnp.bfloat16)
            ahead = routes[level] // rowblocks + level + 1
            target = routes[level] % rowblocks
            held = [] if held is None else held
            held.append((contribution, ahead, target))
            mine = to_chip == chip
            chunks = 0
            for value, value_level, value_row in held:
                hit = mine & (to_row == value_row) & (value_level == level + 1)
                chunks = chunks + jnp.where(hit[:, None, None], value[None].astype(jnp.float32), 0.0)
            received = lax.all_to_all(chunks.astype(jnp.bfloat16), axes, 0, 0, tiled=True)
            received = received.reshape(rowblocks * outer, INNER, nrhs, width)
            incoming[level + 1] = jnp.sum(received.astype(jnp.float32), axis=0)
    return jnp.stack(results, axis=0)[:, None, None]


def solution(mesh):
    return jax.shard_map(
        shards,
        mesh=mesh,
        in_specs=(
            P(None, "rows", "grp", None, None),
            P(None, "rows", "grp", None, None),
            P(None, "rows", "grp", None, None),
            P(None, "rows", "grp", None, None),
            P(None, "rows", "grp"),
        ),
        out_specs=P(None, "rows", "grp", None, None),
        check_vma=False,
    )
```

```python
import functools

import jax
import jax.numpy as jnp
from jax import lax
from jax.experimental import pallas as pl
from jax.experimental.pallas import tpu as pltpu
from jax.sharding import PartitionSpec as P


INNER = 2
F32, BF16 = jnp.float32, jnp.bfloat16


def product(x, w):
    rows = x.shape[0]
    high = x.astype(BF16).astype(F32)
    parts = jnp.concatenate([high, x - high], axis=0).astype(BF16)
    both = jnp.dot(parts, w, preferred_element_type=F32)
    return both[:rows] + both[rows:]


def position():
    group = lax.axis_index("grp")
    return group // INNER, group % INNER


def start_kernel(rhs, inverse, out, first, weight, sem):
    copies = (
        pltpu.make_async_copy(rhs, out, sem.at[0]),
        pltpu.make_async_copy(rhs.at[0], first, sem.at[1]),
        pltpu.make_async_copy(inverse.at[0], weight, sem.at[2]),
    )
    for copy in copies:
        copy.start()
    for copy in copies:
        copy.wait()
    out[0] = product(first[...], weight[...])


def keep_kernel(source, out, sem):
    copy = pltpu.make_async_copy(source, out, sem)
    copy.start()
    copy.wait()


def first_kernel(u, other, inverse, coupler, msg):
    _, core = position()

    @pl.when(core == 1)
    def _():
        msg[...] = u[0] - product(product(other[0], coupler[0]), inverse[0])

    @pl.when(core == 0)
    def _():
        msg[...] = u[0]


def before_kernel(level, received, mine, other, inverse, coupler, inverse_p, coupler_p, msg, own):
    chip, core = position()
    groups = lax.axis_size("grp")
    rowblocks = received.shape[0] // groups
    pair = []
    for which in range(INNER):
        total = received[chip * INNER + which].astype(F32)
        for row in range(1, rowblocks):
            total = total + received[row * groups + chip * INNER + which].astype(F32)
        pair.append(total)

    @pl.when(core == 0)
    def _():
        y = product(mine[level] - pair[0], inverse[level])
        own[...] = y
        msg[...] = product(other[level] - pair[1] - product(y, coupler_p[level]), inverse_p[level])

    @pl.when(core == 1)
    def _():
        y = product(other[level] - pair[0], inverse_p[level])
        y = product(mine[level] - pair[1] - product(y, coupler[level]), inverse[level])
        own[...] = y
        msg[...] = y


def solve(level, own, prev, inverse, coupler, inverse_p, coupler_p, y):
    chip, core = position()
    live = (chip > 0).astype(F32)

    @pl.when(core == 0)
    def _():
        y[...] = own - product(product(live * prev, coupler[level]), inverse[level])

    @pl.when(core == 1)
    def _():
        z = product(product(live * prev, coupler_p[level]), inverse_p[level])
        y[...] = own + product(product(z, coupler[level]), inverse[level])


def after_kernel(level, own, cross, straight, routes, *refs):
    held = refs[: level]
    inverse, coupler, inverse_p, coupler_p, blocks, y, c, chunks = refs[level:]
    chip, core = position()
    groups = lax.axis_size("grp")
    rowblocks = chunks.shape[0] // groups
    prev = cross[...] if straight is None else jnp.where(core == 0, cross[...], straight[...])
    solve(level, own[...], prev, inverse, coupler, inverse_p, coupler_p, y)
    value = jnp.dot(y[...].astype(BF16), blocks[level], preferred_element_type=F32).astype(BF16)
    c[...] = value
    values = [h[...].astype(F32) for h in held] + [value.astype(F32)]
    route = routes[...]
    vectors = [jnp.broadcast_to(route[:, l : l + 1], value.shape) for l in range(level + 1)]
    chunks[...] = jnp.zeros(chunks.shape, chunks.dtype)

    def fill(row, carry):
        chunk = jnp.zeros(value.shape, F32)
        for l in range(level + 1):
            chunk = chunk + jnp.where(vectors[l] == (level - l) * rowblocks + row, values[l], 0.0)
        chunk = chunk.astype(BF16)
        for which in range(INNER):
            chunks[row * groups + chip * INNER + which] = chunk
        return carry

    lax.fori_loop(0, rowblocks, fill, 0, unroll=rowblocks <= 8)


def last_kernel(level, own, cross, inverse, coupler, inverse_p, coupler_p, *refs):
    earlier, out, y = refs[:level], refs[level], refs[level + 1]
    solve(level, own[...], cross[...], inverse, coupler, inverse_p, coupler_p, y)
    for l in range(level):
        out[l] = earlier[l][...]
    out[level] = y[...]


VMEM = pl.BlockSpec(memory_space=pltpu.VMEM)
ANY = pl.BlockSpec(memory_space=pl.ANY)


def call(body, args, out_shape, specs=None, scratch=(), limit=16 * 2**20):
    return pl.pallas_call(
        body,
        out_shape=out_shape,
        in_specs=specs or [VMEM] * len(args),
        out_specs=jax.tree.map(lambda _: VMEM, out_shape),
        scratch_shapes=list(scratch),
        compiler_params=pltpu.CompilerParams(vmem_limit_bytes=limit),
        cost_estimate=pl.CostEstimate(flops=10**6, bytes_accessed=2**20, transcendentals=0),
    )(*args)


def shards(rhs, diag_inverse, coupling, off_block, off_route):
    axes = ("rows", "grp")
    levels, nrhs, width = rhs.shape[0], rhs.shape[3], rhs.shape[4]
    groups, rowblocks = lax.axis_size("grp"), lax.axis_size("rows")
    count = rowblocks * groups
    sides = rhs.reshape(levels, nrhs, width)
    inverse, coupler = diag_inverse.reshape(levels, width, width), coupling.reshape(levels, width, width)
    blocks = off_block.reshape(levels - 1, width, width)
    routes = off_route.reshape(1, levels - 1)

    def moved(value, change):
        return lax.ppermute(value, "grp", [(g, change(g) % groups) for g in range(groups)])

    flip = lambda g: g ^ 1
    straight = lambda g: g + INNER
    cross = lambda g: (g ^ 1) + INNER
    vector = jax.ShapeDtypeStruct((nrhs, width), F32)
    half = jax.ShapeDtypeStruct((nrhs, width), BF16)
    chunk_shape = jax.ShapeDtypeStruct((count, nrhs, width), BF16)

    mine = call(
        start_kernel,
        (sides, inverse),
        jax.ShapeDtypeStruct(sides.shape, F32),
        specs=[ANY, ANY],
        scratch=[pltpu.VMEM((nrhs, width), F32), pltpu.VMEM((width, width), BF16), pltpu.SemaphoreType.DMA((3,))],
    )
    other = moved(mine, flip)
    inverse_p = moved(inverse, flip)
    coupler_p = moved(coupler, flip)
    inverse = call(
        keep_kernel,
        (inverse,),
        jax.ShapeDtypeStruct(inverse.shape, BF16),
        specs=[ANY],
        scratch=[pltpu.SemaphoreType.DMA],
    )
    weights = (inverse, coupler, inverse_p, coupler_p)
    results, contributions, received = [], [], None
    for level in range(levels):
        if level == 0:
            msg = call(first_kernel, (mine, other, inverse, coupler), vector)
            own = msg
        else:
            msg, own = call(
                functools.partial(before_kernel, level), (received, mine, other, *weights), (vector, vector)
            )
        a = moved(msg, cross)
        b = moved(msg, straight) if level == 0 else None
        if level < levels - 1:
            args = (own, a) + ((b,) if level == 0 else ()) + (routes, *contributions, *weights, blocks)
            body = functools.partial(after_kernel, level)
            if level:
                body = lambda own, a, route, *rest, body=body: body(own, a, None, route, *rest)
            y, c, chunks = call(body, args, (vector, half, chunk_shape))
            results.append(y)
            contributions.append(c)
            received = lax.all_to_all(chunks, axes, 0, 0, tiled=True)
        else:
            out = call(
                functools.partial(last_kernel, level),
                (own, a, *weights, *results),
                jax.ShapeDtypeStruct((levels, nrhs, width), F32),
                scratch=[pltpu.VMEM((nrhs, width), F32)],
            )
    return out[:, None, None]


def solution(mesh):
    return jax.shard_map(
        shards,
        mesh=mesh,
        in_specs=(
            P(None, "rows", "grp", None, None),
            P(None, "rows", "grp", None, None),
            P(None, "rows", "grp", None, None),
            P(None, "rows", "grp", None, None),
            P(None, "rows", "grp"),
        ),
        out_specs=P(None, "rows", "grp", None, None),
        check_vma=False,
    )
```
